32 devices in a mesh: dp: 4 (over x, y), tp: 8 (over z, core).
Axes of the slice: x: 2, y: 2, z: 4, core: 2. Of those that a mesh axis runs over, the one named last changes fastest.
Arguments:
- x: bfloat16 [8192, 4096], P('dp'), parts along dimension 0
- w_gate: bfloat16 [4096, 10240], P(None, 'tp')
- w_up: bfloat16 [4096, 10240], P(None, 'tp')
- w_down: bfloat16 [10240, 4096], P('tp')
Outputs:
- output: bfloat16 [8192, 4096], P('dp'), parts along dimension 0
There are 4 independent parts. The reference program is written for one: setup_inputs(seed, part) draws one part's arguments, and reference() takes and returns one part's arrays. A program takes and returns all parts, laid end to end along the dimension named above; an argument that names none is the same for every part.
All inputs are finite; a program needn't handle non-finite values.
Results may differ from the reference program's by a relative error of at most 0.016.
Values are sent between devices in bfloat16 or wider.
A program may use at most 2 GiB of HBM per device.

```python
import jax
import jax.numpy as jnp

ROWS = 2048
D = 4096
FF = 10240


def setup_inputs(seed: int = 0, part: int = 0) -> dict:
    kx, kg, ku, kd = jax.random.split(jax.random.key(seed), 4)
    drawn = {
        "x": jax.random.normal(jax.random.fold_in(kx, part), (ROWS, D), jnp.float32),
        "w_gate": jax.random.normal(kg, (D, FF), jnp.float32) * D**-0.5,
        "w_up": jax.random.normal(ku, (D, FF), jnp.float32) * D**-0.5,
        "w_down": jax.random.normal(kd, (FF, D), jnp.float32) * FF**-0.5,
    }
    return {k: v.astype(jnp.bfloat16) for k, v in drawn.items()}


def reference(x, w_gate, w_up, w_down):
    gate = jnp.dot(x, w_gate, preferred_element_type=jnp.float32)
    up = jnp.dot(x, w_up, preferred_element_type=jnp.float32)
    hidden = (jax.nn.gelu(gate) * up).astype(jnp.bfloat16)
    return jnp.dot(hidden, w_down, preferred_element_type=jnp.float32).astype(jnp.bfloat16)
```

```python
import functools

import jax
import jax.numpy as jnp
from jax import lax
from jax.experimental import pallas as pl
from jax.experimental.pallas import tpu as pltpu
from jax.sharding import PartitionSpec as P

MESH = pl.DeviceIdType.MESH

LANE = 128
PW = 512
HB = 256
RS = 12
RO = 12
SS = 4
LS = 8
LA, LO, LF, LE = 0, 2, 4, 8


def _kernel(cfg, x, wg, wu, wd, y, wgv, wuv, wdv, xb, hid, own, sibr, innr, sst, lst,
            wg_m, wu_m, wd_m, x_m, sib_s, sib_r, lk_s, out_r, inn_r, fin_r, sf_r,
            fs_sib, fs_out, fs_inn, credit):
    rows, d, ff, lane, pw, hb = cfg
    nc, npc, nh = rows // (2 * lane), d // pw, ff // hb
    nq = nc * npc
    me = lax.axis_index("tp")
    z, c = me // 2, me % 2
    end = (z * (3 - z)) == 0
    mid = (z * (3 - z)) != 0
    sib = {"tp": 2 * z + 1 - c}
    inner = {"tp": 2 * (1 + z % 2) + c}
    outer = {"tp": 6 * (z // 2) + c}

    def x_copies(s, slot):
        return [
            pltpu.make_async_copy(
                x.at[pl.ds(pl.multiple_of((2 * s + lax.rem(c + h, 2)) * lane, lane), lane)],
                xb.at[slot, pl.ds(h * lane, lane)], x_m.at[slot, h])
            for h in range(2)
        ]

    def w_copy(src, dst, sem, j, width):
        cols = pl.ds(pl.multiple_of(j * width, width), width)
        return pltpu.make_async_copy(src.at[:, cols], dst.at[:, cols], sem.at[j])

    for cp in x_copies(0, 0):
        cp.start()
    for j in range(nh):
        w_copy(wg, wgv, wg_m, j, hb).start()
        w_copy(wu, wuv, wu_m, j, hb).start()
    for j in range(npc):
        w_copy(wd, wdv, wd_m, j, pw).start()
    for cp in x_copies(1, 1):
        cp.start()

    bar = pltpu.get_barrier_semaphore()
    pl.semaphore_signal(bar, inc=1, device_id=sib, device_id_type=MESH)
    pl.semaphore_signal(bar, inc=1, device_id=inner, device_id_type=MESH)

    @pl.when(mid)
    def _():
        pl.semaphore_signal(bar, inc=1, device_id=outer, device_id_type=MESH)
        pl.semaphore_wait(bar, 3)

    @pl.when(end)
    def _():
        pl.semaphore_wait(bar, 2)

    def at(q, ln):
        s, i = q // npc, q % npc
        return (pl.ds(pl.multiple_of((2 * s + ln) * lane, lane), lane),
                pl.ds(pl.multiple_of(i * pw, pw), pw))

    def remote(src, dst, ss, rs, to):
        return pltpu.make_async_remote_copy(
            src_ref=src, dst_ref=dst, send_sem=ss, recv_sem=rs, device_id=to, device_id_type=MESH)

    def sib_copy(q):
        return remote(sst.at[q % SS], sibr.at[q % RS], sib_s.at[q % SS], sib_r.at[q % RS], sib)

    def end_copy(q):
        r = at(q, c)
        return remote(lst.at[q % LS], y.at[r], lk_s.at[q % LS], out_r.at[q], inner)

    def inn_copy(q):
        k = q // 2
        return remote(lst.at[k % LS], innr.at[k], lk_s.at[k % LS], inn_r.at[k], inner)

    def fin_sib(q):
        r = at(q, c)
        return remote(y.at[r], y.at[r], fs_sib.at[q], sf_r.at[q], sib)

    def fin_out(q):
        r = at(q, c)
        return remote(y.at[r], y.at[r], fs_out.at[q], fin_r.at[q], outer)

    def fin_inn(q):
        r = at(q, c)
        return remote(y.at[r], y.at[r], fs_inn.at[q // 2], fin_r.at[q], inner)

    def sib_fin_in(q):
        r = at(q, 1 - c)
        return remote(y.at[r], y.at[r], fs_sib.at[q], sf_r.at[q], sib)

    def gate_up(s, j):
        slot = s % 2

        @pl.when(j == 0)
        def _():
            for cp in x_copies(s, slot):
                cp.wait()

        @pl.when(s == 0)
        def _():
            w_copy(wg, wgv, wg_m, j, hb).wait()
            w_copy(wu, wuv, wu_m, j, hb).wait()

        cols = pl.ds(pl.multiple_of(j * hb, hb), hb)
        g = jnp.dot(xb[slot], wgv[:, cols], preferred_element_type=jnp.float32)
        u = jnp.dot(xb[slot], wuv[:, cols], preferred_element_type=jnp.float32)
        hid[:, cols] = (jax.nn.gelu(g) * u).astype(jnp.bfloat16)

        @pl.when((j == nh - 1) & (s + 2 < nc))
        def _():
            for cp in x_copies(s + 2, slot):
                cp.start()

    def down(s, i):
        q = s * npc + i

        @pl.when(s == 0)
        def _():
            w_copy(wd, wdv, wd_m, i, pw).wait()

        @pl.when(q >= SS)
        def _():
            sib_copy(q - SS).wait_send()

        cols = pl.ds(pl.multiple_of(i * pw, pw), pw)
        t = jnp.dot(hid[...], wdv[:, cols], preferred_element_type=jnp.float32)
        own[q % RO] = t[:lane]
        sst[q % SS] = t[lane:].astype(jnp.bfloat16)

        @pl.when(q >= RS)
        def _():
            pl.semaphore_wait(credit.at[q % 2], 1)

        sib_copy(q).start()

    def chip_term(q):
        return own[q % RO] + sibr[q % RS].astype(jnp.float32)

    def give_credit(q):
        @pl.when(q + RS < nq)
        def _():
            pl.semaphore_signal(credit.at[q % 2], inc=1, device_id=sib, device_id_type=MESH)

    def send_end(q):
        sib_copy(q).wait_recv()

        @pl.when(q >= LS)
        def _():
            end_copy(q - LS).wait_send()

        lst[q % LS] = chip_term(q).astype(jnp.bfloat16)
        give_credit(q)
        end_copy(q).start()

    def send_inner(q):
        k = q // 2
        sib_copy(q).wait_recv()
        end_copy(q).wait_recv()

        @pl.when(k >= LS)
        def _():
            inn_copy(q - 2 * LS).wait_send()

        lst[k % LS] = (chip_term(q) + y[at(q, c)].astype(jnp.float32)).astype(jnp.bfloat16)
        give_credit(q)
        inn_copy(q).start()

    def finish(q):
        sib_copy(q).wait_recv()
        end_copy(q).wait_recv()
        inn_copy(q).wait_recv()
        r = at(q, c)
        y[r] = (chip_term(q) + y[r].astype(jnp.float32)
                + innr[q // 2].astype(jnp.float32)).astype(jnp.bfloat16)
        give_credit(q)
        fin_inn(q).start()
        fin_out(q).start()
        fin_sib(q).start()

    def inside(q):
        return (q >= 0) & (q < nq)

    def step(it, carry):
        n = it - npc
        s, i = it // npc, it % npc

        @pl.when(mid & inside(n - LA) & ((n - LA + z) % 2 == 0))
        def _():
            send_inner(n - LA)

        @pl.when(mid & inside(n - LO) & ((n - LO + z) % 2 != 0))
        def _():
            finish(n - LO)

        @pl.when(mid & inside(n - LF) & ((n - LF + z) % 2 == 0))
        def _():
            q = n - LF
            fin_inn(q).wait_recv()
            fin_out(q).start()
            fin_sib(q).start()

        @pl.when(end & inside(n - LE))
        def _():
            q = n - LE
            fin_out(q).wait_recv()
            fin_sib(q).start()

        units = nh + npc

        def unit(k, carry):
            w = -(-(units + 1) // npc) * i + k

            @pl.when((s < nc) & (w < nh))
            def _():
                gate_up(s, w)

            @pl.when((s < nc) & (w >= nh) & (w < units))
            def _():
                down(s, w - nh)

            @pl.when(end & (s < nc) & (w > nh) & (w <= units))
            def _():
                send_end(s * npc + w - nh - 1)

            return carry

        lax.fori_loop(0, -(-(units + 1) // npc), unit, 0)
        return carry

    lax.fori_loop(0, npc + nq + max(LA, LO, LF, LE), step, 0)

    def drain(q, carry):
        sib_fin_in(q).wait_recv()
        fin_sib(q).wait_send()

        @pl.when(mid)
        def _():
            fin_out(q).wait_send()

        @pl.when(mid & ((q + z) % 2 != 0))
        def _():
            fin_inn(q).wait_send()

        @pl.when(q >= nq - SS)
        def _():
            sib_copy(q).wait_send()

        @pl.when(end & (q >= nq - LS))
        def _():
            end_copy(q).wait_send()

        @pl.when(mid & (q >= nq - 2 * LS) & ((q + z) % 2 == 0))
        def _():
            inn_copy(q).wait_send()

        return carry

    lax.fori_loop(0, nq, drain, 0)


def block(x, w_gate, w_up, w_down, lane=LANE, pw=PW, hb=HB):
    rows, d = x.shape
    ff = w_gate.shape[1]
    nq = rows // (2 * lane) * (d // pw)
    bf, f32 = jnp.bfloat16, jnp.float32
    dma = pltpu.SemaphoreType.DMA
    return pl.pallas_call(
        functools.partial(_kernel, (rows, d, ff, lane, pw, hb)),
        out_shape=pltpu.VMEM((rows, d), bf),
        in_specs=[pl.BlockSpec(memory_space=pl.ANY)] * 4,
        out_specs=pl.BlockSpec(memory_space=pltpu.VMEM),
        scratch_shapes=[
            pltpu.VMEM((d, ff), bf),
            pltpu.VMEM((d, ff), bf),
            pltpu.VMEM((ff, d), bf),
            pltpu.VMEM((2, 2 * lane, d), bf),
            pltpu.VMEM((2 * lane, ff), bf),
            pltpu.VMEM((RO, lane, pw), f32),
            pltpu.VMEM((RS, lane, pw), bf),
            pltpu.VMEM((nq // 2, lane, pw), bf),
            pltpu.VMEM((SS, lane, pw), bf),
            pltpu.VMEM((LS, lane, pw), bf),
            dma((ff // hb,)), dma((ff // hb,)), dma((d // pw,)), dma((2, 2)),
            dma((SS,)), dma((RS,)), dma((LS,)),
            dma((nq,)), dma((nq // 2,)), dma((nq,)), dma((nq,)),
            dma((nq,)), dma((nq,)), dma((nq // 2,)),
            pltpu.SemaphoreType.REGULAR((2,)),
        ],
        compiler_params=pltpu.CompilerParams(
            collective_id=0, has_side_effects=True, vmem_limit_bytes=48 * 2**20 - 64 * 1024),
    )(x, w_gate, w_up, w_down)


def solution(mesh):
    return jax.shard_map(
        block,
        mesh=mesh,
        in_specs=(P("dp", None), P(None, "tp"), P(None, "tp"), P("tp", None)),
        out_specs=P("dp", None),
        check_vma=False,
    )
```

```python
import functools

import jax
import jax.numpy as jnp
from jax import lax
from jax.experimental import pallas as pl
from jax.experimental.pallas import tpu as pltpu
from jax.sharding import PartitionSpec as P

MESH = pl.DeviceIdType.MESH

LANE = 128
PW = 512
HB = 256
RS = 12
RO = 12
SS = 4
LS = 8
AHEAD = 2
LA, LO, LF, LE, LD = 0, 2, 4, 8, 10


def _kernel(cfg, x, wg, wu, wd, y, wgv, wuv, wdv, xb, hid, own, sibr, innr, sst, lst,
            wg_m, wu_m, wd_m, x_m, sib_s, sib_r, lk_s, out_r, inn_r, fin_r, sf_r,
            fs_sib, fs_out, fs_inn, credit):
    rows, d, ff, lane, pw, hb = cfg
    nc, npc, nh = rows // (2 * lane), d // pw, ff // hb
    nq = nc * npc
    me = lax.axis_index("tp")
    z, c = me // 2, me % 2
    end = (z * (3 - z)) == 0
    mid = (z * (3 - z)) != 0
    sib = {"tp": 2 * z + 1 - c}
    inner = {"tp": 2 * (1 + z % 2) + c}
    outer = {"tp": 6 * (z // 2) + c}

    def x_copies(s, slot):
        return [
            pltpu.make_async_copy(
                x.at[pl.ds(pl.multiple_of((2 * s + lax.rem(c + h, 2)) * lane, lane), lane)],
                xb.at[slot, pl.ds(h * lane, lane)], x_m.at[slot, h])
            for h in range(2)
        ]

    def w_copy(src, dst, sem, j, width):
        cols = pl.ds(pl.multiple_of(j * width, width), width)
        return pltpu.make_async_copy(src.at[:, cols], dst.at[:, cols], sem.at[j])

    for cp in x_copies(0, 0):
        cp.start()
    for j in range(AHEAD):
        w_copy(wg, wgv, wg_m, j, hb).start()
        w_copy(wu, wuv, wu_m, j, hb).start()

    bar = pltpu.get_barrier_semaphore()
    pl.semaphore_signal(bar, inc=1, device_id=sib, device_id_type=MESH)
    pl.semaphore_signal(bar, inc=1, device_id=inner, device_id_type=MESH)

    @pl.when(mid)
    def _():
        pl.semaphore_signal(bar, inc=1, device_id=outer, device_id_type=MESH)
        pl.semaphore_wait(bar, 3)

    @pl.when(end)
    def _():
        pl.semaphore_wait(bar, 2)

    def at(q, ln):
        s, i = q // npc, q % npc
        return (pl.ds(pl.multiple_of((2 * s + ln) * lane, lane), lane),
                pl.ds(pl.multiple_of(i * pw, pw), pw))

    def remote(src, dst, ss, rs, to):
        return pltpu.make_async_remote_copy(
            src_ref=src, dst_ref=dst, send_sem=ss, recv_sem=rs, device_id=to, device_id_type=MESH)

    def sib_copy(q):
        return remote(sst.at[q % SS], sibr.at[q % RS], sib_s.at[q % SS], sib_r.at[q % RS], sib)

    def end_copy(q):
        r = at(q, c)
        return remote(lst.at[q % LS], y.at[r], lk_s.at[q % LS], out_r.at[q], inner)

    def inn_copy(q):
        k = q // 2
        return remote(lst.at[k % LS], innr.at[k], lk_s.at[k % LS], inn_r.at[k], inner)

    def fin_sib(q):
        r = at(q, c)
        return remote(y.at[r], y.at[r], fs_sib.at[q], sf_r.at[q], sib)

    def fin_out(q):
        r = at(q, c)
        return remote(y.at[r], y.at[r], fs_out.at[q], fin_r.at[q], outer)

    def fin_inn(q):
        r = at(q, c)
        return remote(y.at[r], y.at[r], fs_inn.at[q // 2], fin_r.at[q], inner)

    def sib_fin_in(q):
        r = at(q, 1 - c)
        return remote(y.at[r], y.at[r], fs_sib.at[q], sf_r.at[q], sib)

    def gate_up(s, j):
        slot = s % 2

        @pl.when(j == 0)
        def _():
            for cp in x_copies(s, slot):
                cp.wait()

        @pl.when(s == 0)
        def _():
            w_copy(wg, wgv, wg_m, j, hb).wait()
            w_copy(wu, wuv, wu_m, j, hb).wait()

            @pl.when(j + AHEAD < nh)
            def _():
                w_copy(wg, wgv, wg_m, j + AHEAD, hb).start()
                w_copy(wu, wuv, wu_m, j + AHEAD, hb).start()

            @pl.when(j + AHEAD == nh)
            def _():
                for i in range(npc):
                    w_copy(wd, wdv, wd_m, i, pw).start()

        @pl.when((s == 0) & (j == nh - 1))
        def _():
            for cp in x_copies(1, 1):
                cp.start()

        cols = pl.ds(pl.multiple_of(j * hb, hb), hb)
        g = jnp.dot(xb[slot], wgv[:, cols], preferred_element_type=jnp.float32)
        u = jnp.dot(xb[slot], wuv[:, cols], preferred_element_type=jnp.float32)
        hid[:, cols] = (jax.nn.gelu(g) * u).astype(jnp.bfloat16)

        @pl.when((j == nh - 1) & (s + 2 < nc))
        def _():
            for cp in x_copies(s + 2, slot):
                cp.start()

    def down(s, i):
        q = s * npc + i

        @pl.when(s == 0)
        def _():
            w_copy(wd, wdv, wd_m, i, pw).wait()

        @pl.when(q >= SS)
        def _():
            sib_copy(q - SS).wait_send()

        cols = pl.ds(pl.multiple_of(i * pw, pw), pw)
        t = jnp.dot(hid[...], wdv[:, cols], preferred_element_type=jnp.float32)
        own[q % RO] = t[:lane]
        sst[q % SS] = t[lane:].astype(jnp.bfloat16)

        @pl.when(q >= RS)
        def _():
            pl.semaphore_wait(credit.at[q % 2], 1)

        sib_copy(q).start()

    def chip_term(q):
        return own[q % RO] + sibr[q % RS].astype(jnp.float32)

    def give_credit(q):
        @pl.when(q + RS < nq)
        def _():
            pl.semaphore_signal(credit.at[q % 2], inc=1, device_id=sib, device_id_type=MESH)

    def send_end(q):
        sib_copy(q).wait_recv()

        @pl.when(q >= LS)
        def _():
            end_copy(q - LS).wait_send()

        lst[q % LS] = chip_term(q).astype(jnp.bfloat16)
        give_credit(q)
        end_copy(q).start()

    def send_inner(q):
        k = q // 2
        sib_copy(q).wait_recv()
        end_copy(q).wait_recv()

        @pl.when(k >= LS)
        def _():
            inn_copy(q - 2 * LS).wait_send()

        lst[k % LS] = (chip_term(q) + y[at(q, c)].astype(jnp.float32)).astype(jnp.bfloat16)
        give_credit(q)
        inn_copy(q).start()

    def finish(q):
        sib_copy(q).wait_recv()
        end_copy(q).wait_recv()
        inn_copy(q).wait_recv()
        r = at(q, c)
        y[r] = (chip_term(q) + y[r].astype(jnp.float32)
                + innr[q // 2].astype(jnp.float32)).astype(jnp.bfloat16)
        give_credit(q)
        fin_inn(q).start()
        fin_out(q).start()
        fin_sib(q).start()

    def drain(q):
        sib_fin_in(q).wait_recv()
        fin_sib(q).wait_send()

        @pl.when(mid)
        def _():
            fin_out(q).wait_send()

        @pl.when(mid & ((q + z + c) % 2 != 0))
        def _():
            fin_inn(q).wait_send()

        @pl.when(q >= nq - SS)
        def _():
            sib_copy(q).wait_send()

        @pl.when(end & (q >= nq - LS))
        def _():
            end_copy(q).wait_send()

        @pl.when(mid & (q >= nq - 2 * LS) & ((q + z + c) % 2 == 0))
        def _():
            inn_copy(q).wait_send()

    def inside(q):
        return (q >= 0) & (q < nq)

    def step(it, carry):
        n = it - npc
        s, i = it // npc, it % npc

        @pl.when(mid & inside(n - LA) & ((n - LA + z + c) % 2 == 0))
        def _():
            send_inner(n - LA)

        @pl.when(mid & inside(n - LO) & ((n - LO + z + c) % 2 != 0))
        def _():
            finish(n - LO)

        @pl.when(mid & inside(n - LF) & ((n - LF + z + c) % 2 == 0))
        def _():
            q = n - LF
            fin_inn(q).wait_recv()
            fin_out(q).start()
            fin_sib(q).start()

        @pl.when(end & inside(n - LE))
        def _():
            q = n - LE
            fin_out(q).wait_recv()
            fin_sib(q).start()

        @pl.when(inside(n - LD))
        def _():
            drain(n - LD)

        units = nh + npc
        gap = max(1, npc // (nh + 3))
        per = -(-(npc + 1) // (npc - nh * gap))

        def unit(k, carry):
            w = jnp.where(i < nh * gap, jnp.where((k == 0) & (i % gap == 0), i // gap, units + 1),
                          nh + per * (i - nh * gap) + k)

            @pl.when((s < nc) & (w < nh))
            def _():
                gate_up(s, w)

            @pl.when((s < nc) & (w >= nh) & (w < units))
            def _():
                down(s, w - nh)

            @pl.when(end & (s < nc) & (w > nh) & (w <= units))
            def _():
                send_end(s * npc + w - nh - 1)

            return carry

        lax.fori_loop(0, per, unit, 0)
        return carry

    lax.fori_loop(0, npc + nq + LD, step, 0)


def block(x, w_gate, w_up, w_down, lane=LANE, pw=PW, hb=HB):
    rows, d = x.shape
    ff = w_gate.shape[1]
    nq = rows // (2 * lane) * (d // pw)
    bf, f32 = jnp.bfloat16, jnp.float32
    dma = pltpu.SemaphoreType.DMA
    return pl.pallas_call(
        functools.partial(_kernel, (rows, d, ff, lane, pw, hb)),
        out_shape=pltpu.VMEM((rows, d), bf),
        in_specs=[pl.BlockSpec(memory_space=pl.ANY)] * 4,
        out_specs=pl.BlockSpec(memory_space=pltpu.VMEM),
        scratch_shapes=[
            pltpu.VMEM((d, ff), bf),
            pltpu.VMEM((d, ff), bf),
            pltpu.VMEM((ff, d), bf),
            pltpu.VMEM((2, 2 * lane, d), bf),
            pltpu.VMEM((2 * lane, ff), bf),
            pltpu.VMEM((RO, lane, pw), f32),
            pltpu.VMEM((RS, lane, pw), bf),
            pltpu.VMEM((nq // 2, lane, pw), bf),
            pltpu.VMEM((SS, lane, pw), bf),
            pltpu.VMEM((LS, lane, pw), bf),
            dma((ff // hb,)), dma((ff // hb,)), dma((d // pw,)), dma((2, 2)),
            dma((SS,)), dma((RS,)), dma((LS,)),
            dma((nq,)), dma((nq // 2,)), dma((nq,)), dma((nq,)),
            dma((nq,)), dma((nq,)), dma((nq // 2,)),
            pltpu.SemaphoreType.REGULAR((2,)),
        ],
        compiler_params=pltpu.CompilerParams(
            collective_id=0, has_side_effects=True, vmem_limit_bytes=48 * 2**20 - 64 * 1024),
    )(x, w_gate, w_up, w_down)


def solution(mesh):
    return jax.shard_map(
        block,
        mesh=mesh,
        in_specs=(P("dp", None), P(None, "tp"), P(None, "tp"), P("tp", None)),
        out_specs=P("dp", None),
        check_vma=False,
    )
```

```python
import functools

import jax
import jax.numpy as jnp
from jax import lax
from jax.experimental import pallas as pl
from jax.experimental.pallas import tpu as pltpu
from jax.sharding import PartitionSpec as P

MESH = pl.DeviceIdType.MESH

LANE = 128
PW = 512
HB = 256
RS = 12
RO = 12
SS = 4
LS = 8
AHEAD = 2
QS, H = 4, 2
LA, LO, LF, LE, LD = 0, 2, 4, 8, 10


def _kernel(cfg, x, wg, wu, wd, y, wgv, wuv, wdv, xb, hid, own, sibr, innr, sst, lst,
            wg_m, wu_m, wd_m, x_m, sib_s, sib_r, lk_s, out_r, inn_r, fin_r, sf_r,
            fs_sib, fs_out, fs_inn, credit):
    rows, d, ff, lane, pw, hb = cfg
    nc, npc, nh = rows // (2 * lane), d // pw, ff // hb
    nq = nc * npc
    me = lax.axis_index("tp")
    z, c = me // 2, me % 2
    end = (z * (3 - z)) == 0
    mid = (z * (3 - z)) != 0
    sib = {"tp": 2 * z + 1 - c}
    inner = {"tp": 2 * (1 + z % 2) + c}
    outer = {"tp": 6 * (z // 2) + c}

    def x_copies(s, slot):
        return [
            pltpu.make_async_copy(
                x.at[pl.ds(pl.multiple_of((2 * s + lax.rem(c + h, 2)) * lane, lane), lane)],
                xb.at[slot, pl.ds(h * lane, lane)], x_m.at[slot, h])
            for h in range(2)
        ]

    def w_copy(src, dst, sem, j, width):
        cols = pl.ds(pl.multiple_of(j * width, width), width)
        return pltpu.make_async_copy(src.at[:, cols], dst.at[:, cols], sem.at[j])

    for cp in x_copies(0, 0):
        cp.start()
    for j in range(AHEAD):
        w_copy(wg, wgv, wg_m, j, hb).start()
        w_copy(wu, wuv, wu_m, j, hb).start()

    bar = pltpu.get_barrier_semaphore()
    pl.semaphore_signal(bar, inc=1, device_id=sib, device_id_type=MESH)
    pl.semaphore_signal(bar, inc=1, device_id=inner, device_id_type=MESH)

    @pl.when(mid)
    def _():
        pl.semaphore_signal(bar, inc=1, device_id=outer, device_id_type=MESH)
        pl.semaphore_wait(bar, 3)

    @pl.when(end)
    def _():
        pl.semaphore_wait(bar, 2)

    def at(q, ln):
        s, i = q // npc, q % npc
        return (pl.ds(pl.multiple_of((2 * s + ln) * lane, lane), lane),
                pl.ds(pl.multiple_of(i * pw, pw), pw))

    def remote(src, dst, ss, rs, to):
        return pltpu.make_async_remote_copy(
            src_ref=src, dst_ref=dst, send_sem=ss, recv_sem=rs, device_id=to, device_id_type=MESH)

    def sib_copy(q):
        return remote(sst.at[q % SS], sibr.at[q % RS], sib_s.at[q % SS], sib_r.at[q % RS], sib)

    def rows_of(h, n):
        return pl.ds(h * (lane // n), lane // n)

    def part(q, h, n):
        r, cols = at(q, c)
        return pl.ds(pl.multiple_of(r.start + h * (lane // n), lane // n), lane // n), cols

    def sem(arr, base, k, h):
        return arr.at[k if h == 0 else base + k * (H - 1) + h - 1]

    def split(q, fn):
        @pl.when(q < QS)
        def _():
            for h in range(H):
                fn(h, H)

        @pl.when(q >= QS)
        def _():
            fn(0, 1)

    def end_copy(q, h, n):
        r = part(q, h, n)
        return remote(lst.at[q % LS, rows_of(h, n)], y.at[r], sem(lk_s, LS, q % LS, h),
                      sem(out_r, nq, q, h), inner)

    def inn_copy(q, h, n):
        k = q // 2
        return remote(lst.at[k % LS, rows_of(h, n)], innr.at[k, rows_of(h, n)],
                      sem(lk_s, LS, k % LS, h), sem(inn_r, nq // 2, k, h), inner)

    def fin_sib(q):
        r = at(q, c)
        return remote(y.at[r], y.at[r], fs_sib.at[q], sf_r.at[q], sib)

    def fin_out(q, h, n):
        r = part(q, h, n)
        return remote(y.at[r], y.at[r], sem(fs_out, nq, q, h), sem(fin_r, nq, q, h), outer)

    def fin_inn(q, h, n):
        r = part(q, h, n)
        return remote(y.at[r], y.at[r], sem(fs_inn, nq // 2, q // 2, h), sem(fin_r, nq, q, h), inner)

    def sib_fin_in(q):
        r = at(q, 1 - c)
        return remote(y.at[r], y.at[r], fs_sib.at[q], sf_r.at[q], sib)

    def gate_up(s, j):
        slot = s % 2

        @pl.when(j == 0)
        def _():
            for cp in x_copies(s, slot):
                cp.wait()

        @pl.when(s == 0)
        def _():
            w_copy(wg, wgv, wg_m, j, hb).wait()
            w_copy(wu, wuv, wu_m, j, hb).wait()

            @pl.when(j + AHEAD < nh)
            def _():
                w_copy(wg, wgv, wg_m, j + AHEAD, hb).start()
                w_copy(wu, wuv, wu_m, j + AHEAD, hb).start()

            @pl.when(j + AHEAD == nh)
            def _():
                for i in range(npc):
                    w_copy(wd, wdv, wd_m, i, pw).start()

        @pl.when((s == 0) & (j == nh - 1))
        def _():
            for cp in x_copies(1, 1):
                cp.start()

        cols = pl.ds(pl.multiple_of(j * hb, hb), hb)
        g = jnp.dot(xb[slot], wgv[:, cols], preferred_element_type=jnp.float32)
        u = jnp.dot(xb[slot], wuv[:, cols], preferred_element_type=jnp.float32)
        hid[:, cols] = (jax.nn.gelu(g) * u).astype(jnp.bfloat16)

        @pl.when((j == nh - 1) & (s + 2 < nc))
        def _():
            for cp in x_copies(s + 2, slot):
                cp.start()

    def down(s, i):
        q = s * npc + i

        @pl.when(s == 0)
        def _():
            w_copy(wd, wdv, wd_m, i, pw).wait()

        @pl.when(q >= SS)
        def _():
            sib_copy(q - SS).wait_send()

        cols = pl.ds(pl.multiple_of(i * pw, pw), pw)
        t = jnp.dot(hid[...], wdv[:, cols], preferred_element_type=jnp.float32)
        own[q % RO] = t[:lane]
        sst[q % SS] = t[lane:].astype(jnp.bfloat16)

        @pl.when(q >= RS)
        def _():
            pl.semaphore_wait(credit.at[q % 2], 1)

        sib_copy(q).start()

    def chip_term(q, h, n):
        return own[q % RO, rows_of(h, n)] + sibr[q % RS, rows_of(h, n)].astype(jnp.float32)

    def give_credit(q):
        @pl.when(q + RS < nq)
        def _():
            pl.semaphore_signal(credit.at[q % 2], inc=1, device_id=sib, device_id_type=MESH)

    def send_end(q):
        sib_copy(q).wait_recv()

        @pl.when(q >= LS)
        def _():
            split(q - LS, lambda h, n: end_copy(q - LS, h, n).wait_send())

        def go(h, n):
            lst[q % LS, rows_of(h, n)] = chip_term(q, h, n).astype(jnp.bfloat16)
            end_copy(q, h, n).start()

        split(q, go)
        give_credit(q)

    def send_inner(q):
        k = q // 2
        sib_copy(q).wait_recv()

        @pl.when(k >= LS)
        def _():
            split(q - 2 * LS, lambda h, n: inn_copy(q - 2 * LS, h, n).wait_send())

        def go(h, n):
            end_copy(q, h, n).wait_recv()
            lst[k % LS, rows_of(h, n)] = (
                chip_term(q, h, n) + y[part(q, h, n)].astype(jnp.float32)).astype(jnp.bfloat16)
            inn_copy(q, h, n).start()

        split(q, go)
        give_credit(q)

    def finish(q):
        sib_copy(q).wait_recv()

        def go(h, n):
            end_copy(q, h, n).wait_recv()
            inn_copy(q, h, n).wait_recv()
            r = part(q, h, n)
            y[r] = (chip_term(q, h, n) + y[r].astype(jnp.float32)
                    + innr[q // 2, rows_of(h, n)].astype(jnp.float32)).astype(jnp.bfloat16)
            fin_inn(q, h, n).start()
            fin_out(q, h, n).start()

        split(q, go)
        give_credit(q)
        fin_sib(q).start()

    def forward(q):
        def go(h, n):
            fin_inn(q, h, n).wait_recv()
            fin_out(q, h, n).start()

        split(q, go)
        fin_sib(q).start()

    def drain(q):
        sib_fin_in(q).wait_recv()
        fin_sib(q).wait_send()

        @pl.when(mid)
        def _():
            split(q, lambda h, n: fin_out(q, h, n).wait_send())

        @pl.when(mid & ((q + z + c) % 2 != 0))
        def _():
            split(q, lambda h, n: fin_inn(q, h, n).wait_send())

        @pl.when(q >= nq - SS)
        def _():
            sib_copy(q).wait_send()

        @pl.when(end & (q >= nq - LS))
        def _():
            end_copy(q, 0, 1).wait_send()

        @pl.when(mid & (q >= nq - 2 * LS) & ((q + z + c) % 2 == 0))
        def _():
            inn_copy(q, 0, 1).wait_send()

    def inside(q):
        return (q >= 0) & (q < nq)

    def step(it, carry):
        n = it - npc
        s, i = it // npc, it % npc

        @pl.when(mid & inside(n - LA) & ((n - LA + z + c) % 2 == 0))
        def _():
            send_inner(n - LA)

        @pl.when(mid & inside(n - LO) & ((n - LO + z + c) % 2 != 0))
        def _():
            finish(n - LO)

        @pl.when(mid & inside(n - LF) & ((n - LF + z + c) % 2 == 0))
        def _():
            forward(n - LF)

        @pl.when(end & inside(n - LE))
        def _():
            q = n - LE
            split(q, lambda h, n: fin_out(q, h, n).wait_recv())
            fin_sib(q).start()

        @pl.when(inside(n - LD))
        def _():
            drain(n - LD)

        units = nh + npc
        gap = max(1, npc // (nh + 3))
        per = -(-(npc + 1) // (npc - nh * gap))

        def unit(k, carry):
            w = jnp.where(i < nh * gap, jnp.where((k == 0) & (i % gap == 0), i // gap, units + 1),
                          nh + per * (i - nh * gap) + k)

            @pl.when((s < nc) & (w < nh))
            def _():
                gate_up(s, w)

            @pl.when((s < nc) & (w >= nh) & (w < units))
            def _():
                down(s, w - nh)

            @pl.when(end & (s < nc) & (w > nh) & (w <= units))
            def _():
                send_end(s * npc + w - nh - 1)

            return carry

        lax.fori_loop(0, per, unit, 0)
        return carry

    lax.fori_loop(0, npc + nq + LD, step, 0)


def block(x, w_gate, w_up, w_down, lane=LANE, pw=PW, hb=HB):
    rows, d = x.shape
    ff = w_gate.shape[1]
    nq = rows // (2 * lane) * (d // pw)
    bf, f32 = jnp.bfloat16, jnp.float32
    more = QS * (H - 1)
    dma = pltpu.SemaphoreType.DMA
    return pl.pallas_call(
        functools.partial(_kernel, (rows, d, ff, lane, pw, hb)),
        out_shape=pltpu.VMEM((rows, d), bf),
        in_specs=[pl.BlockSpec(memory_space=pl.ANY)] * 4,
        out_specs=pl.BlockSpec(memory_space=pltpu.VMEM),
        scratch_shapes=[
            pltpu.VMEM((d, ff), bf),
            pltpu.VMEM((d, ff), bf),
            pltpu.VMEM((ff, d), bf),
            pltpu.VMEM((2, 2 * lane, d), bf),
            pltpu.VMEM((2 * lane, ff), bf),
            pltpu.VMEM((RO, lane, pw), f32),
            pltpu.VMEM((RS, lane, pw), bf),
            pltpu.VMEM((nq // 2, lane, pw), bf),
            pltpu.VMEM((SS, lane, pw), bf),
            pltpu.VMEM((LS, lane, pw), bf),
            dma((ff // hb,)), dma((ff // hb,)), dma((d // pw,)), dma((2, 2)),
            dma((SS,)), dma((RS,)), dma((LS * H,)),
            dma((nq + more,)), dma((nq // 2 + more,)), dma((nq + more,)), dma((nq,)),
            dma((nq,)), dma((nq + more,)), dma((nq // 2 + more,)),
            pltpu.SemaphoreType.REGULAR((2,)),
        ],
        compiler_params=pltpu.CompilerParams(
            collective_id=0, has_side_effects=True, vmem_limit_bytes=48 * 2**20 - 64 * 1024),
    )(x, w_gate, w_up, w_down)


def solution(mesh):
    return jax.shard_map(
        block,
        mesh=mesh,
        in_specs=(P("dp", None), P(None, "tp"), P(None, "tp"), P("tp", None)),
        out_specs=P("dp", None),
        check_vma=False,
    )
```
